32 devices in a mesh: shard: 8 (over z, y), tp: 4 (over x, core).
Axes of the slice: x: 2, y: 2, z: 4, core: 2. Of those that a mesh axis runs over, the one named last changes fastest.
Arguments:
- weight_query: bfloat16 [12288, 12288], P('shard', 'tp'), may hold values from -0.078125 to 0.078125
- low_query: bfloat16 [12288, 64], P('shard'), may hold values from -0.0546875 to 0.0546875
- high_query: bfloat16 [64, 12288], P(None, 'tp'), may hold values from -0.75 to 0.75
- weight_key: bfloat16 [12288, 12288], P('shard', 'tp'), may hold values from -0.078125 to 0.078125
- low_key: bfloat16 [12288, 64], P('shard'), may hold values from -0.0546875 to 0.0546875
- high_key: bfloat16 [64, 12288], P(None, 'tp'), may hold values from -0.75 to 0.75
- weight_value: bfloat16 [12288, 12288], P('shard', 'tp'), may hold values from -0.078125 to 0.078125
- low_value: bfloat16 [12288, 64], P('shard'), may hold values from -0.0546875 to 0.0546875
- high_value: bfloat16 [64, 12288], P(None, 'tp'), may hold values from -0.75 to 0.75
- norm_train: float32 [12288], P(('shard', 'tp')), may hold values from 0.25 to 1.75
- norm_step: float32 [12288], P(('shard', 'tp')), may hold values from -0.3 to 0.3
Outputs:
- ready_query: bfloat16 [12288, 12288], P(None, ('tp', 'shard'))
- ready_key: bfloat16 [12288, 12288], P(None, ('tp', 'shard'))
- ready_value: bfloat16 [12288, 12288], P(None, ('tp', 'shard'))
- column_query: float32 [12288], P(('tp', 'shard'))
- column_key: float32 [12288], P(('tp', 'shard'))
- column_value: float32 [12288], P(('tp', 'shard'))
- serve_norm: bfloat16 [12288], replicated
The draws below stay inside these ranges and needn't reach their ends.
All inputs are finite; a program needn't handle non-finite values. Where the reference program divides by a largest or mean magnitude, that divisor is 1e-20 or more.
Results may differ from the reference program's by a relative error of at most 0.001.
Values may be sent and summed in bfloat16 or wider, within the bound.
A program may use at most 192 MiB of HBM per device.

```python
import jax
import jax.numpy as jnp

D_MODEL = 12288
Q_DIM = 12288
KV_DIM = 12288
RANK = 64


def with_spikes(values, key, source, target, parts, factor):
    owner, partner = [(jnp.arange(values.shape[position]) // (values.shape[position] // parts)).reshape([-1 if axis == position else 1 for axis in range(values.ndim)]) for position in (source, target)]
    chosen = jax.random.permutation(key, parts)[partner]
    strong = (owner == chosen) | (owner == (partner + parts // 2) % parts)
    return jnp.where(strong, factor * values, values)


def levels(stream_key, dims, shards, smallest, largest):
    loudness = 1.0
    for dim, parts in shards:
        draws = jax.random.uniform(jax.random.fold_in(jax.random.fold_in(stream_key, 6), dim), (parts,), jnp.float32, smallest / len(shards), largest / len(shards))
        loudness = loudness * jnp.repeat(jnp.exp(draws), dims[dim] // parts).reshape((-1,) + (1,) * (len(dims) - 1 - dim))
    return loudness


def bell_draw(key, extent, spread, bound, cuts=(), kind=jnp.bfloat16):
    loudness = levels(key, extent, cuts, -0.22, 0.18) if cuts else 1.0
    values = jax.random.normal(key, extent, jnp.float32) * spread * loudness
    return jnp.minimum(jnp.maximum(values, -bound), bound).astype(kind)


def heavy_noise(key, extent, width, most, shards, heavy, kind=jnp.bfloat16):
    array = width * jax.random.normal(key, extent, jnp.float32)
    if shards:
        array = array * levels(key, extent, shards, -0.22, 0.18)
    return jnp.clip(with_spikes(array, jax.random.fold_in(key, 3), *heavy), -most, most).astype(kind)


def setup_inputs(seed: int = 0) -> dict:
    seeds = jax.random.split(jax.random.key(seed), 12)
    return {
        "weight_query": heavy_noise(seeds[0], (D_MODEL, Q_DIM), D_MODEL ** -0.5, 0.078125, ((0, 8), (1, 4)), (0, 1, 8, 2.0)),
        "low_query": bell_draw(seeds[1], (D_MODEL, RANK), D_MODEL ** -0.5, 0.0546875, ((0, 8),)),
        "high_query": bell_draw(seeds[2], (RANK, Q_DIM), RANK ** -0.5, 0.75, ((1, 4),)),
        "weight_key": heavy_noise(seeds[3], (D_MODEL, KV_DIM), D_MODEL ** -0.5, 0.078125, ((0, 8), (1, 4)), (0, 1, 8, 2.0)),
        "low_key": bell_draw(seeds[4], (D_MODEL, RANK), D_MODEL ** -0.5, 0.0546875, ((0, 8),)),
        "high_key": bell_draw(seeds[5], (RANK, KV_DIM), RANK ** -0.5, 0.75, ((1, 4),)),
        "weight_value": heavy_noise(seeds[6], (D_MODEL, KV_DIM), D_MODEL ** -0.5, 0.078125, ((0, 8), (1, 4)), (0, 1, 8, 2.0)),
        "low_value": bell_draw(seeds[7], (D_MODEL, RANK), D_MODEL ** -0.5, 0.0546875, ((0, 8),)),
        "high_value": bell_draw(seeds[8], (RANK, KV_DIM), RANK ** -0.5, 0.75, ((1, 4),)),
        "norm_train": jnp.clip(1.0 + 0.15 * jax.random.normal(seeds[9], (D_MODEL,), jnp.float32), 0.25, 1.75),
        "norm_step": jnp.clip(jax.random.uniform(seeds[10], (D_MODEL,), jnp.float32, -0.3, 0.3) * levels(seeds[10], (D_MODEL,), ((0, 32),), -0.4, 0.0), -0.3, 0.3),
    }


mix_rate = 0.5


def reference(weight_query, low_query, high_query, weight_key, low_key, high_key, weight_value, low_value, high_value, norm_train, norm_step):
    latest_query = weight_query.astype(jnp.float32) + mix_rate * jnp.dot(low_query, high_query, preferred_element_type=jnp.float32)
    latest_key = weight_key.astype(jnp.float32) + mix_rate * jnp.dot(low_key, high_key, preferred_element_type=jnp.float32)
    latest_value = weight_value.astype(jnp.float32) + mix_rate * jnp.dot(low_value, high_value, preferred_element_type=jnp.float32)
    column_query = jnp.sum(jnp.abs(latest_query), axis=0) / D_MODEL
    ready_query = (latest_query / column_query).astype(jnp.bfloat16)
    column_key = jnp.sum(jnp.abs(latest_key), axis=0) / D_MODEL
    ready_key = (latest_key / column_key).astype(jnp.bfloat16)
    column_value = jnp.sum(jnp.abs(latest_value), axis=0) / D_MODEL
    ready_value = (latest_value / column_value).astype(jnp.bfloat16)
    serve_norm = (norm_train + norm_step).astype(jnp.bfloat16)
    return ready_query, ready_key, ready_value, column_query, column_key, column_value, serve_norm
```

```python
import functools

import jax
import jax.numpy as jnp
from jax import lax
from jax.experimental import pallas as pl
from jax.experimental.pallas import tpu as pltpu
from jax.sharding import PartitionSpec as P

mix_rate = 0.5
MESH = pl.DeviceIdType.MESH
TILE = 256
RAW = 128
CHUNK = 128
SPLIT = 96


def merged(weight, low, high):
    product = jnp.dot(low, high, preferred_element_type=jnp.float32)
    return weight.astype(jnp.float32) + mix_rate * product


def exchange(
    n, parts, depth,
    wq, wk, wv, lq, lk, lv, hq, hk, hv, train, step,
    land_q, land_k, land_v, col, norm,
    wbuf, ltbuf, lbuf, hbuf, part, stat, raw, rawlow, gains,
    load_sem, high_sem, low_sem, gain_sem,
    send_sem, recv_sem, part_send, part_recv, col_send, col_recv,
    raw_send, raw_recv,
    rlow_send, rlow_recv, norm_send, norm_recv, side_send, side_recv,
):
    weights, lows, highs = (wq, wk, wv), (lq, lk, lv), (hq, hk, hv)
    lands = (land_q, land_k, land_v)
    rows, width = wbuf.shape[2], wbuf.shape[3]
    me, side = lax.axis_index("shard"), lax.axis_index("tp")
    half, pairs = n // 2, n // 4
    top, place, odd = me // half, me % half, me % 2
    own = n - 1

    def target(k):
        flip = lax.rem(odd + k % 2, 2)
        if k < half:
            return 2 * (top * (k // 2) + (1 - top) * (n // 2 - 1 - k // 2)) + flip
        j = (k - half) // 2 + 1
        if j < pairs:
            return 2 * (top * pairs + lax.rem(place // 2 + j, pairs)) + flip
        return me if k == own else me + 1 - 2 * odd

    def cols(k):
        return pl.ds(pl.multiple_of(target(k) * width, 128), width)

    def shifted(d):
        return lax.rem(me + d, n)

    order = list(range(n))
    loads = {}
    for m in range(3):
        loads[m] = pltpu.make_async_copy(lows[m], ltbuf.at[m], low_sem.at[m])
        for k in order:
            loads[m, k] = (
                pltpu.make_async_copy(highs[m].at[:, cols(k)], hbuf.at[m, k], high_sem.at[m, k]),
                pltpu.make_async_copy(weights[m].at[:, cols(k)], wbuf.at[m, k], load_sem.at[m, k]),
            )

    def fetch(m):
        loads[m].start()
        for k in order:
            for copy in loads[m, k]:
                copy.start()

    fetch(0)
    gain_loads = [
        pltpu.make_async_copy(source, gains.at[i], gain_sem.at[i]) for i, source in enumerate((train, step))
    ]
    for copy in gain_loads:
        copy.start()

    barrier = pltpu.get_barrier_semaphore()
    for d in range(1, n):
        pl.semaphore_signal(barrier, inc=1, device_id={"shard": shifted(d)}, device_id_type=MESH)
    for j in range(1, parts):
        pl.semaphore_signal(
            barrier, inc=1, device_id={"tp": lax.rem(side + j, parts)}, device_id_type=MESH
        )
    pl.semaphore_wait(barrier, n - 1 + parts - 1)

    def remote(src, dst, send, recv, device):
        copy = pltpu.make_async_remote_copy(
            src_ref=src, dst_ref=dst, send_sem=send, recv_sem=recv,
            device_id=device, device_id_type=MESH,
        )
        copy.start()
        return copy

    def raw_part(p, k, here):
        at = pl.ds(*((0, SPLIT), (SPLIT, RAW - SPLIT))[p])
        return pltpu.make_async_remote_copy(
            src_ref=wv.at[at, cols(k)], dst_ref=raw.at[here, at],
            send_sem=raw_send.at[p, k], recv_sem=raw_recv.at[p, here],
            device_id={"shard": target(k)}, device_id_type=MESH,
        )

    def raw_low(k, here):
        return pltpu.make_async_remote_copy(
            src_ref=lv.at[:, pl.ds(0, RAW)], dst_ref=rawlow.at[here],
            send_sem=rlow_send.at[k], recv_sem=rlow_recv.at[here],
            device_id={"shard": target(k)}, device_id_type=MESH,
        )

    for k in range(half):
        raw_part(0, k, place).start()
    def sums(m):
        loads[m].wait()
        lbuf[m] = jnp.transpose(ltbuf[m].astype(jnp.float32)).astype(jnp.bfloat16)
        for k in order:
            for copy in loads[m, k]:
                copy.wait()

            def tile(i, total):
                at = pl.ds(pl.multiple_of(i * TILE, TILE), TILE)
                latest = merged(wbuf[m, k, at, :], lbuf[m, at, :], hbuf[m, k])
                return total + jnp.sum(jnp.abs(latest), axis=0, keepdims=True)

            part[m, k] = lax.fori_loop(0, rows // TILE, tile, jnp.zeros((1, width), jnp.float32))
        for k in range(own):
            part_copy(m, k, me).start()

    def part_copy(m, k, source):
        return pltpu.make_async_remote_copy(
            src_ref=part.at[m, k], dst_ref=stat.at[m, source],
            send_sem=part_send.at[m, k], recv_sem=part_recv.at[m, source],
            device_id={"shard": target(k)}, device_id_type=MESH,
        )

    def columns(m):
        total = part[m, own]
        for d in range(1, n):
            source = shifted(d)
            part_copy(m, 0, source).wait_recv()
            total = total + stat[m, source]
        total = total / depth
        col[m, me] = total
        return [
            remote(col.at[m, me], col.at[m, me], col_send.at[m, d], col_recv.at[m, d], {"shard": shifted(d)})
            for d in range(1, n)
        ]

    def settle(copies):
        for copy in copies:
            copy.wait()

    def block_copy(m, k, first, count, source):
        return pltpu.make_async_remote_copy(
            src_ref=wbuf.at[m, k, pl.ds(first, count)],
            dst_ref=lands[m].at[pl.ds(pl.multiple_of(source * rows + first, 16), count)],
            send_sem=send_sem.at[m, k], recv_sem=recv_sem.at[m, source],
            device_id={"shard": target(k)}, device_id_type=MESH,
        )

    def ready(m, start, stop):
        def chunk(slots, i, carry):
            first = pl.multiple_of(i * CHUNK, CHUNK)
            at = pl.ds(first, CHUNK)
            behind = None
            for k in slots:
                latest = merged(wbuf[m, k, at, :], lbuf[m, at, :], hbuf[m, k])
                narrow = (latest / col[m, target(k)]).astype(jnp.bfloat16)
                if k == own:
                    lands[m][pl.ds(pl.multiple_of(me * rows + first, CHUNK), CHUNK), :] = narrow
                else:
                    wbuf[m, k, at, :] = narrow
                if behind is not None:
                    block_copy(m, behind, first, CHUNK, me).start()
                behind = k
            return carry

        near = list(range(half, own))
        mixed = []
        for k in range(half):
            mixed.append(k)
            mixed.extend(near[k:k + 1])
        begin = max(start, RAW // CHUNK) if m == 2 else start
        lax.fori_loop(start, begin, functools.partial(chunk, near + [own]), 0)
        lax.fori_loop(begin, stop, functools.partial(chunk, mixed + [own]), 0)

    chunks = rows // CHUNK
    early = chunks // 4
    chunks = rows // CHUNK
    early = chunks // 4
    sums(0)
    for k in range(half):
        raw_part(1, k, place).start()
        raw_low(k, place).start()
    fetch(1)
    scales = columns(0)
    settle(scales)
    ready(0, 0, early)
    for copy in gain_loads:
        copy.wait()
    norm[me, side, 0, :] = gains[0] + gains[1]
    sums(1)
    fetch(2)
    norms = [
        remote(norm.at[me, side], norm.at[me, side], norm_send.at[d], norm_recv.at[d], {"shard": shifted(d)})
        for d in range(1, n)
    ]
    ready(0, early, 2 * early)
    scales = columns(1)
    sums(2)
    ready(0, 2 * early, 3 * early)
    later = columns(2)
    ready(0, 3 * early, chunks)
    settle(scales)
    ready(1, 0, chunks)
    settle(later)
    ready(2, 0, chunks)

    for copy in norms:
        copy.wait()
    sides = [
        remote(norm.at[:, side], norm.at[:, side], side_send.at[j], side_recv.at[j], {"tp": lax.rem(side + j, parts)})
        for j in range(1, parts)
    ]

    for i in range(half):
        for p in range(2):
            raw_part(p, 0, i).wait_recv()
        raw_low(0, i).wait_recv()
        low = jnp.transpose(rawlow[i].astype(jnp.float32)).astype(jnp.bfloat16)
        latest = merged(raw[i], low, hbuf[2, own])
        source = (1 - top) * half + i
        land_v[pl.ds(pl.multiple_of(source * rows, RAW), RAW), :] = (latest / col[2, me]).astype(jnp.bfloat16)

    for copy in sides:
        copy.wait()
    for k in range(half):
        for p in range(2):
            raw_part(p, k, place).wait_send()
        raw_low(k, place).wait_send()
    for m in range(3):
        for k in range(own):
            part_copy(m, k, me).wait_send()
            first = RAW if m == 2 and k < half else 0
            block_copy(m, k, first, rows - first, me).wait_send()
        for i in range(half):
            first = RAW if m == 2 else 0
            block_copy(m, 0, first, rows - first, (1 - top) * half + i).wait_recv()
        for d in range(1, half):
            block_copy(m, half, 0, rows, top * half + lax.rem(place + d, half)).wait_recv()


def finish(q_in, k_in, v_in, col, norm, q_out, k_out, v_out, q_col, k_col, v_col, serve, sem):
    copies = [
        pltpu.make_async_copy(source, out, sem.at[m])
        for m, (source, out) in enumerate(((q_in, q_out), (k_in, k_out), (v_in, v_out)))
    ]
    for copy in copies:
        copy.start()
    me = lax.axis_index("shard")
    for m, out in enumerate((q_col, k_col, v_col)):
        out[...] = col[m, me, 0, :]
    n, parts, _, piece = norm.shape
    for s in range(n):
        for t in range(parts):
            serve[pl.ds((s * parts + t) * piece, piece)] = norm[s, t, 0, :].astype(jnp.bfloat16)
    for copy in copies:
        copy.wait()


def kernel_body(
    n, parts,
    weight_query, low_query, high_query,
    weight_key, low_key, high_key,
    weight_value, low_value, high_value,
    norm_train, norm_step,
):
    rows, wide = weight_query.shape
    width, depth = wide // n, rows * n
    rank, piece = low_query.shape[1], norm_train.shape[0]
    anywhere = pl.BlockSpec(memory_space=pl.ANY)
    vmem = pl.BlockSpec(memory_space=pltpu.VMEM)
    land = pltpu.VMEM((depth, width), jnp.bfloat16)
    dma = pltpu.SemaphoreType.DMA
    half = n // 2
    gathered = pl.pallas_call(
        functools.partial(exchange, n, parts, depth),
        out_shape=(
            land, land, land,
            pltpu.VMEM((3, n, 1, width), jnp.float32),
            pltpu.VMEM((n, parts, 1, piece), jnp.float32),
        ),
        in_specs=[anywhere] * 11,
        out_specs=(vmem,) * 5,
        scratch_shapes=[
            pltpu.VMEM((3, n, rows, width), jnp.bfloat16),
            pltpu.VMEM((3, rank, rows), jnp.bfloat16),
            pltpu.VMEM((3, rows, rank), jnp.bfloat16),
            pltpu.VMEM((3, n, rank, width), jnp.bfloat16),
            pltpu.VMEM((3, n, 1, width), jnp.float32),
            pltpu.VMEM((3, n, 1, width), jnp.float32),
            pltpu.VMEM((half, RAW, width), jnp.bfloat16),
            pltpu.VMEM((half, rank, RAW), jnp.bfloat16),
            pltpu.VMEM((2, piece), jnp.float32),
            dma((3, n)), dma((3, n)), dma((3,)), dma((2,)),
            dma((3, n)), dma((3, n)), dma((3, n)), dma((3, n)), dma((3, n)), dma((3, n)),
            dma((2, half)), dma((2, half)), dma((half,)), dma((half,)),
            dma((n,)), dma((n,)), dma((parts,)), dma((parts,)),
        ],
        compiler_params=pltpu.CompilerParams(
            collective_id=0, has_side_effects=True, vmem_limit_bytes=35 * 2**20
        ),
        name="exchange",
    )(
        weight_query, weight_key, weight_value,
        low_query.T, low_key.T, low_value.T,
        high_query, high_key, high_value,
        norm_train, norm_step,
    )
    ready = jax.ShapeDtypeStruct((depth, width), jnp.bfloat16)
    column = jax.ShapeDtypeStruct((width,), jnp.float32)
    return pl.pallas_call(
        finish,
        out_shape=(
            (ready,) * 3 + (column,) * 3
            + (jax.ShapeDtypeStruct((n * parts * piece,), jnp.bfloat16),)
        ),
        in_specs=[anywhere] * 3 + [vmem] * 2,
        out_specs=(anywhere,) * 3 + (vmem,) * 4,
        scratch_shapes=[dma((3,))],
        compiler_params=pltpu.CompilerParams(vmem_limit_bytes=2**20),
        name="finish",
    )(*gathered)


def plain_body(
    weight_query, low_query, high_query,
    weight_key, low_key, high_key,
    weight_value, low_value, high_value,
    norm_train, norm_step,
):
    n = lax.axis_size("shard")
    latest = [
        merged(weight, low, high)
        for weight, low, high in (
            (weight_query, low_query, high_query),
            (weight_key, low_key, high_key),
            (weight_value, low_value, high_value),
        )
    ]
    totals = lax.psum(tuple(jnp.sum(jnp.abs(x), axis=0) for x in latest), "shard")
    place = lax.axis_index("shard")
    readies, columns = [], []
    for x, total in zip(latest, totals):
        column = total / (x.shape[0] * n)
        narrow = (x / column).astype(jnp.bfloat16)
        ready = lax.all_to_all(narrow, "shard", split_axis=1, concat_axis=0, tiled=True)
        readies.append(ready)
        columns.append(lax.dynamic_slice_in_dim(column, place * ready.shape[1], ready.shape[1]))
    serve = (norm_train + norm_step).astype(jnp.bfloat16)
    serve = lax.all_gather(serve, ("shard", "tp"), tiled=True)
    return (*readies, *columns, serve)


def solution(mesh):
    n, parts = mesh.shape["shard"], mesh.shape["tp"]

    def body(*args):
        rows, wide = args[0].shape
        fits = (
            n % 4 == 0
            and wide % (n * 128) == 0
            and rows % TILE == 0
            and rows % CHUNK == 0
            and all(args[i].shape == args[0].shape for i in (3, 6))
            and 6 * rows * wide < 40 * 2**20
        )
        if fits:
            return kernel_body(n, parts, *args)
        return plain_body(*args)

    weight, low, high = P("shard", "tp"), P("shard", None), P(None, "tp")
    norm = P(("shard", "tp"))
    ready, column = P(None, ("tp", "shard")), P(("tp", "shard"))
    return jax.shard_map(
        body,
        mesh=mesh,
        in_specs=(weight, low, high) * 3 + (norm, norm),
        out_specs=(ready,) * 3 + (column,) * 3 + (P(),),
        check_vma=False,
    )
```

```python
import functools

import jax
import jax.numpy as jnp
from jax import lax
from jax.experimental import pallas as pl
from jax.experimental.pallas import tpu as pltpu
from jax.sharding import PartitionSpec as P

mix_rate = 0.5
MESH = pl.DeviceIdType.MESH
TILE = 256
CHUNK = 128
RAW_PARTS = (160, 48, 48)
RAW = sum(RAW_PARTS)
EXTRA = 512
PIECES = 4


def merged(weight, low, high):
    product = jnp.dot(low, high, preferred_element_type=jnp.float32)
    return weight.astype(jnp.float32) + mix_rate * product


def places(n):
    me = lax.axis_index("shard")
    half, pairs = n // 2, n // 4
    top, place, odd = me // half, me % half, me % 2

    def target(k):
        flip = lax.rem(odd + k % 2, 2)
        if k < half:
            return 2 * (top * (k // 2) + (1 - top) * (n // 2 - 1 - k // 2)) + flip
        j = (k - half) // 2 + 1
        if j < pairs:
            return 2 * (top * pairs + lax.rem(place // 2 + j, pairs)) + flip
        return me if k == n - 1 else me + 1 - 2 * odd

    return me, half, top, place, target


def interleaved(half, own):
    near = list(range(half, own))
    mixed = []
    for k in range(half):
        mixed.append(k)
        mixed.extend(near[k:k + 1])
    return mixed


def exchange(
    n, parts, depth,
    wq, wk, wv, lq, lk, lv, hq, hk, hv, train, step,
    land_q, land_k, later, head, col, norm,
    wbuf, ltbuf, lbuf, hbuf, part, stat, raw, rawlow, gains,
    load_sem, high_sem, low_sem, gain_sem,
    send_sem, recv_sem, part_send, part_recv, col_send, col_recv,
    raw_send, raw_recv, rlow_send, rlow_recv, spread_send, spread_recv,
    norm_send, norm_recv, side_send, side_recv, extra_send, extra_recv,
):
    weights, lows, highs = (wq, wk, wv), (lq, lk, lv), (hq, hk, hv)
    lands = (land_q, land_k)
    rows, width = later.shape[1], later.shape[2]
    me, half, top, place, target = places(n)
    side = lax.axis_index("tp")
    own = n - 1
    share = rawlow.shape[1] // parts

    def block(m, k):
        return later.at[k] if m == 2 else wbuf.at[m, k]

    def cols(k):
        return pl.ds(pl.multiple_of(target(k) * width, 128), width)

    def shifted(d):
        return lax.rem(me + d, n)

    order = list(range(n))
    loads = {}
    for m in range(3):
        loads[m] = pltpu.make_async_copy(lows[m], ltbuf.at[m], low_sem.at[m])
        for k in order:
            loads[m, k] = (
                pltpu.make_async_copy(highs[m].at[:, cols(k)], hbuf.at[m, k], high_sem.at[m, k]),
                pltpu.make_async_copy(weights[m].at[:, cols(k)], block(m, k), load_sem.at[m, k]),
            )

    def fetch(m):
        loads[m].start()
        for k in order:
            for copy in loads[m, k]:
                copy.start()

    fetch(0)
    gain_loads = [
        pltpu.make_async_copy(source, gains.at[i], gain_sem.at[i]) for i, source in enumerate((train, step))
    ]
    for copy in gain_loads:
        copy.start()

    barrier = pltpu.get_barrier_semaphore()
    for d in range(1, n):
        pl.semaphore_signal(barrier, inc=1, device_id={"shard": shifted(d)}, device_id_type=MESH)
    for j in range(1, parts):
        pl.semaphore_signal(
            barrier, inc=1, device_id={"tp": lax.rem(side + j, parts)}, device_id_type=MESH
        )
    pl.semaphore_wait(barrier, n - 1 + parts - 1)

    def remote(src, dst, send, recv, device):
        return pltpu.make_async_remote_copy(
            src_ref=src, dst_ref=dst, send_sem=send, recv_sem=recv,
            device_id=device, device_id_type=MESH,
        )

    def begun(copies):
        for copy in copies:
            copy.start()
        return copies

    def settle(copies):
        for copy in copies:
            copy.wait()

    def raw_part(p, k, here):
        at = pl.ds(sum(RAW_PARTS[:p]), RAW_PARTS[p])
        return remote(
            wv.at[at, cols(k)], raw.at[here, at], raw_send.at[p, k], raw_recv.at[p, here], {"shard": target(k)}
        )

    def raw_low(k, here):
        mine = pl.ds(pl.multiple_of(side * share, share), share)
        return remote(
            lv.at[mine, pl.ds(0, RAW)], rawlow.at[here, mine], rlow_send.at[k], rlow_recv.at[here],
            {"shard": target(k)},
        )

    def send_raw(p):
        for k in range(half):
            raw_part(p, k, place).start()

    def part_copy(m, k, source):
        return remote(
            part.at[m, k], stat.at[m, source], part_send.at[m, k], part_recv.at[m, source], {"shard": target(k)}
        )

    def sums(m):
        loads[m].wait()
        lbuf[m] = jnp.transpose(ltbuf[m].astype(jnp.float32)).astype(jnp.bfloat16)
        for k in order:
            for copy in loads[m, k]:
                copy.wait()

            def tile(i, total):
                at = pl.ds(pl.multiple_of(i * TILE, TILE), TILE)
                latest = merged(block(m, k)[at, :], lbuf[m, at, :], hbuf[m, k])
                return total + jnp.sum(jnp.abs(latest).reshape(TILE // 8, 8, width), axis=0)

            total = lax.fori_loop(0, rows // TILE, tile, jnp.zeros((8, width), jnp.float32))
            part[m, k] = jnp.sum(total, axis=0, keepdims=True)
        for k in range(own):
            part_copy(m, k, me).start()

    def columns(m):
        total = part[m, own]
        for d in range(1, n):
            source = shifted(d)
            part_copy(m, 0, source).wait_recv()
            total = total + stat[m, source]
        col[m, me] = total / depth
        return begun([
            remote(col.at[m, me], col.at[m, me], col_send.at[m, d], col_recv.at[m, d], {"shard": shifted(d)})
            for d in range(1, n)
        ])

    def block_copy(m, k, first, count, source):
        return remote(
            wbuf.at[m, k, pl.ds(first, count)],
            lands[m].at[pl.ds(pl.multiple_of(source * rows + first, 16), count)],
            send_sem.at[m, k], recv_sem.at[m, source], {"shard": target(k)},
        )

    mixed = interleaved(half, own)

    def ready(m, start, stop):
        def chunk(i, carry):
            first = pl.multiple_of(i * CHUNK, CHUNK)
            at = pl.ds(first, CHUNK)
            behind = None
            for k in mixed + [own]:
                latest = merged(block(m, k)[at, :], lbuf[m, at, :], hbuf[m, k])
                narrow = (latest / col[m, target(k)]).astype(jnp.bfloat16)
                if m < 2 and k == own:
                    lands[m][pl.ds(pl.multiple_of(me * rows + first, CHUNK), CHUNK), :] = narrow
                else:
                    block(m, k)[at, :] = narrow
                if m < 2 and behind is not None:
                    block_copy(m, behind, first, CHUNK, me).start()
                behind = k
            return carry

        lax.fori_loop(start, stop, chunk, 0)

    def extra_copy(k, here, first, count):
        return remote(
            later.at[k, pl.ds(first, count)], head.at[here, pl.ds(first, count)],
            extra_send.at[k], extra_recv.at[here], {"shard": target(k)},
        )

    chunks = rows // CHUNK
    early = chunks // 4
    send_raw(0)
    sums(0)
    send_raw(1)
    fetch(1)
    scales = columns(0)
    send_raw(2)
    begun([raw_low(k, place) for k in range(half)])
    settle(scales)
    ready(0, 0, early)
    settle(gain_loads)
    norm[me, side, 0, :] = gains[0] + gains[1]
    sums(1)
    fetch(2)
    norms = begun([
        remote(norm.at[me, side], norm.at[me, side], norm_send.at[d], norm_recv.at[d], {"shard": shifted(d)})
        for d in range(1, n)
    ])
    ready(0, early, 2 * early)
    scales = columns(1)
    sums(2)
    ready(0, 2 * early, 3 * early)
    last = columns(2)
    ready(0, 3 * early, chunks)
    for i in range(half):
        raw_low(0, i).wait_recv()
    mine = pl.ds(pl.multiple_of(side * share, share), share)
    spreads = begun([
        remote(
            rawlow.at[:, mine], rawlow.at[:, mine], spread_send.at[j], spread_recv.at[j],
            {"tp": lax.rem(side + j, parts)},
        )
        for j in range(1, parts)
    ])
    settle(scales)
    ready(1, 0, chunks)
    settle(last)
    ready(2, 0, chunks)

    @pl.when(side % 2 == 1)
    def _():
        def more(i, carry):
            first = pl.multiple_of(i * CHUNK, CHUNK)
            for k in range(half):
                extra_copy(k, place, first, CHUNK).start()
            return carry

        lax.fori_loop(RAW // CHUNK, (RAW + EXTRA) // CHUNK, more, 0)

    settle(norms)
    sides = begun([
        remote(norm.at[:, side], norm.at[:, side], side_send.at[j], side_recv.at[j], {"tp": lax.rem(side + j, parts)})
        for j in range(1, parts)
    ])
    settle(spreads)
    for i in range(half):
        for p in range(len(RAW_PARTS)):
            raw_part(p, 0, i).wait_recv()
        low = jnp.transpose(rawlow[i].astype(jnp.float32)).astype(jnp.bfloat16)
        latest = merged(raw[i], low, hbuf[2, own])
        head[i, pl.ds(0, RAW), :] = (latest / col[2, me]).astype(jnp.bfloat16)
    settle(sides)

    for k in range(half):
        for p in range(len(RAW_PARTS)):
            raw_part(p, k, place).wait_send()
        raw_low(k, place).wait_send()
    for k in range(own):
        for m in range(3):
            part_copy(m, k, me).wait_send()
        for m in range(2):
            block_copy(m, k, 0, rows, me).wait_send()
    for m in range(2):
        for d in range(1, n):
            block_copy(m, 0, 0, rows, shifted(d)).wait_recv()

    @pl.when(side % 2 == 1)
    def _():
        for i in range(half):
            extra_copy(i, place, RAW, EXTRA).wait_send()
            extra_copy(0, i, RAW, EXTRA).wait_recv()


def exchange_value(n, later, _, land, send_sem, recv_sem):
    rows = later.shape[1]
    me, half, top, place, target = places(n)
    parity = lax.axis_index("tp") % 2
    own = n - 1
    barrier = pltpu.get_barrier_semaphore()
    for d in range(1, n):
        pl.semaphore_signal(
            barrier, inc=1, device_id={"shard": lax.rem(me + d, n)}, device_id_type=MESH
        )
    pl.semaphore_wait(barrier, n - 1)

    def block_copy(k, first, count, source):
        return pltpu.make_async_remote_copy(
            src_ref=later.at[k, pl.ds(first, count)],
            dst_ref=land.at[pl.ds(pl.multiple_of(source * rows + first, 16), count)],
            send_sem=send_sem.at[k], recv_sem=recv_sem.at[source],
            device_id={"shard": target(k)}, device_id_type=MESH,
        )

    chunks = rows // CHUNK
    near = list(range(half, own))
    for odd in range(2):
        skip = RAW + odd * EXTRA

        @pl.when(parity == odd)
        def _():
            def both(i, carry):
                first = pl.multiple_of(i * CHUNK, CHUNK)
                for k in interleaved(half, own):
                    block_copy(k, first + skip if k < half else first, CHUNK, me).start()
                return carry

            def rest(i, carry):
                for k in near:
                    block_copy(k, pl.multiple_of(i * CHUNK, CHUNK), CHUNK, me).start()
                return carry

            far = chunks - skip // CHUNK
            lax.fori_loop(0, far, both, 0)
            lax.fori_loop(far, chunks, rest, 0)
            for k in range(own):
                first = skip if k < half else 0
                block_copy(k, first, rows - first, me).wait_send()
            for i in range(half):
                block_copy(0, skip, rows - skip, (1 - top) * half + i).wait_recv()
            for d in range(1, half):
                block_copy(half, 0, rows, top * half + lax.rem(place + d, half)).wait_recv()


def finish(q_in, k_in, col, norm, q_out, k_out, q_col, k_col, v_col, serve, sem):
    step = q_in.shape[0] // PIECES
    copies = [
        pltpu.make_async_copy(source.at[pl.ds(i * step, step)], out.at[pl.ds(i * step, step)], sem.at[m, i])
        for m, (source, out) in enumerate(((q_in, q_out), (k_in, k_out)))
        for i in range(PIECES)
    ]
    for copy in copies:
        copy.start()
    me = lax.axis_index("shard")
    for m, out in enumerate((q_col, k_col, v_col)):
        out[...] = col[m, me, 0, :]
    n, parts, _, piece = norm.shape
    for s in range(n):
        for t in range(parts):
            serve[pl.ds((s * parts + t) * piece, piece)] = norm[s, t, 0, :].astype(jnp.bfloat16)
    for copy in copies:
        copy.wait()


def finish_value(n, land, head, later, out, own_sem, near_sem, head_sem, extra_sem, far_sem):
    rows = later.shape[1]
    me, half, top, place, _ = places(n)
    parity = lax.axis_index("tp") % 2

    def at(source, first, count):
        return pl.ds(pl.multiple_of(source * rows + first, 16), count)

    def moved(source, first, count, sem):
        here = at(source, first, count)
        return pltpu.make_async_copy(land.at[here], out.at[here], sem)

    def kept(i, source, first, count, sem):
        return pltpu.make_async_copy(head.at[i, pl.ds(first, count)], out.at[at(source, first, count)], sem)

    copies = [pltpu.make_async_copy(later.at[n - 1], out.at[at(me, 0, rows)], own_sem)]
    for d in range(1, half):
        copies.append(moved(top * half + lax.rem(place + d, half), 0, rows, near_sem.at[d]))
    split = RAW + EXTRA
    sources = [(1 - top) * half + i for i in range(half)]
    for i, source in enumerate(sources):
        copies.append(kept(i, source, 0, RAW, head_sem.at[i]))
        copies.append(moved(source, split, rows - split, far_sem.at[i]))
    for copy in copies:
        copy.start()

    @pl.when(parity == 0)
    def _():
        for i, source in enumerate(sources):
            moved(source, RAW, EXTRA, extra_sem.at[i]).start()

    @pl.when(parity == 1)
    def _():
        for i, source in enumerate(sources):
            kept(i, source, RAW, EXTRA, extra_sem.at[i]).start()

    for i, source in enumerate(sources):
        copies.append(moved(source, RAW, EXTRA, extra_sem.at[i]))
    for copy in copies:
        copy.wait()


def kernel_body(
    n, parts,
    weight_query, low_query, high_query,
    weight_key, low_key, high_key,
    weight_value, low_value, high_value,
    norm_train, norm_step,
):
    rows, wide = weight_query.shape
    width, depth = wide // n, rows * n
    rank, piece = low_query.shape[1], norm_train.shape[0]
    anywhere = pl.BlockSpec(memory_space=pl.ANY)
    vmem = pl.BlockSpec(memory_space=pltpu.VMEM)
    land = pltpu.VMEM((depth, width), jnp.bfloat16)
    later = pltpu.VMEM((n, rows, width), jnp.bfloat16)
    dma = pltpu.SemaphoreType.DMA
    half = n // 2
    land_q, land_k, value, head, col, norm = pl.pallas_call(
        functools.partial(exchange, n, parts, depth),
        out_shape=(
            land, land, later,
            pltpu.VMEM((half, RAW + EXTRA, width), jnp.bfloat16),
            pltpu.VMEM((3, n, 1, width), jnp.float32),
            pltpu.VMEM((n, parts, 1, piece), jnp.float32),
        ),
        in_specs=[anywhere] * 11,
        out_specs=(vmem,) * 6,
        scratch_shapes=[
            pltpu.VMEM((2, n, rows, width), jnp.bfloat16),
            pltpu.VMEM((3, rank, rows), jnp.bfloat16),
            pltpu.VMEM((3, rows, rank), jnp.bfloat16),
            pltpu.VMEM((3, n, rank, width), jnp.bfloat16),
            pltpu.VMEM((3, n, 1, width), jnp.float32),
            pltpu.VMEM((3, n, 1, width), jnp.float32),
            pltpu.VMEM((half, RAW, width), jnp.bfloat16),
            pltpu.VMEM((half, rank, RAW), jnp.bfloat16),
            pltpu.VMEM((2, piece), jnp.float32),
            dma((3, n)), dma((3, n)), dma((3,)), dma((2,)),
            dma((2, n)), dma((2, n)), dma((3, n)), dma((3, n)), dma((3, n)), dma((3, n)),
            dma((len(RAW_PARTS), half)), dma((len(RAW_PARTS), half)),
            dma((half,)), dma((half,)), dma((parts,)), dma((parts,)),
            dma((n,)), dma((n,)), dma((parts,)), dma((parts,)), dma((half,)), dma((half,)),
        ],
        compiler_params=pltpu.CompilerParams(
            collective_id=0, has_side_effects=True, vmem_limit_bytes=28 * 2**20
        ),
        name="exchange",
    )(
        weight_query, weight_key, weight_value,
        low_query.T, low_key.T, low_value.T,
        high_query, high_key, high_value,
        norm_train, norm_step,
    )
    ready = jax.ShapeDtypeStruct((depth, width), jnp.bfloat16)
    column = jax.ShapeDtypeStruct((width,), jnp.float32)
    ready_q, ready_k, col_q, col_k, col_v, serve = pl.pallas_call(
        finish,
        out_shape=(
            (ready,) * 2 + (column,) * 3
            + (jax.ShapeDtypeStruct((n * parts * piece,), jnp.bfloat16),)
        ),
        in_specs=[anywhere] * 2 + [vmem] * 2,
        out_specs=(anywhere,) * 2 + (vmem,) * 4,
        scratch_shapes=[dma((2, PIECES))],
        compiler_params=pltpu.CompilerParams(vmem_limit_bytes=2**20),
        name="finish",
    )(land_q, land_k, col, norm)
    land_v = pl.pallas_call(
        functools.partial(exchange_value, n),
        out_shape=land,
        in_specs=[vmem, anywhere],
        out_specs=vmem,
        scratch_shapes=[dma((n,)), dma((n,))],
        compiler_params=pltpu.CompilerParams(
            collective_id=1, has_side_effects=True, vmem_limit_bytes=2**20
        ),
        name="exchange_value",
    )(value, col_q)
    ready_v = pl.pallas_call(
        functools.partial(finish_value, n),
        out_shape=ready,
        in_specs=[anywhere] * 3,
        out_specs=anywhere,
        scratch_shapes=[dma(()), dma((half,)), dma((half,)), dma((half,)), dma((half,))],
        compiler_params=pltpu.CompilerParams(vmem_limit_bytes=2**20),
        name="finish_value",
    )(land_v, head, value)
    return (ready_q, ready_k, ready_v, col_q, col_k, col_v, serve)


def plain_body(
    weight_query, low_query, high_query,
    weight_key, low_key, high_key,
    weight_value, low_value, high_value,
    norm_train, norm_step,
):
    n = lax.axis_size("shard")
    latest = [
        merged(weight, low, high)
        for weight, low, high in (
            (weight_query, low_query, high_query),
            (weight_key, low_key, high_key),
            (weight_value, low_value, high_value),
        )
    ]
    totals = lax.psum(tuple(jnp.sum(jnp.abs(x), axis=0) for x in latest), "shard")
    place = lax.axis_index("shard")
    readies, columns = [], []
    for x, total in zip(latest, totals):
        column = total / (x.shape[0] * n)
        narrow = (x / column).astype(jnp.bfloat16)
        ready = lax.all_to_all(narrow, "shard", split_axis=1, concat_axis=0, tiled=True)
        readies.append(ready)
        columns.append(lax.dynamic_slice_in_dim(column, place * ready.shape[1], ready.shape[1]))
    serve = (norm_train + norm_step).astype(jnp.bfloat16)
    serve = lax.all_gather(serve, ("shard", "tp"), tiled=True)
    return (*readies, *columns, serve)


def solution(mesh):
    n, parts = mesh.shape["shard"], mesh.shape["tp"]

    def body(*args):
        rows, wide = args[0].shape
        fits = (
            n % 4 == 0
            and wide % (n * 128) == 0
            and rows % TILE == 0
            and rows % (4 * CHUNK) == 0
            and rows > RAW + EXTRA
            and args[1].shape[1] % (16 * parts) == 0
            and rows * n % PIECES == 0
            and all(args[i].shape == args[0].shape for i in (3, 6))
            and 6 * rows * wide < 40 * 2**20
        )
        if fits:
            return kernel_body(n, parts, *args)
        return plain_body(*args)

    weight, low, high = P("shard", "tp"), P("shard", None), P(None, "tp")
    norm = P(("shard", "tp"))
    ready, column = P(None, ("tp", "shard")), P(("tp", "shard"))
    return jax.shard_map(
        body,
        mesh=mesh,
        in_specs=(weight, low, high) * 3 + (norm, norm),
        out_specs=(ready,) * 3 + (column,) * 3 + (P(),),
        check_vma=False,
    )
```
